32 devices in a mesh: freq: 4 (over y, x), band: 8 (over z, core).
Axes of the slice: x: 2, y: 2, z: 4, core: 2. Of those that a mesh axis runs over, the one named last changes fastest.
Arguments:
- pair_density: bfloat16 [1024, 2, 8192], P(('freq', 'band')), may hold values from -6 to 6
- trial_vectors: bfloat16 [16, 2, 64, 8192], P('freq', None, None, 'band'), may hold values from -6 to 6
- frequency: float32 [16], P('freq'), may hold values from 0.05 to 20
- val_energy: float32 [32], replicated, may hold values from -3 to -0.1
- cond_energy: float32 [32], replicated, may hold values from 0.1 to 4
- pair_index: int32 [1024], P(('freq', 'band')), may hold values from 0 to 1023, each once
Outputs:
- images: float32 [16, 2, 64, 8192], P('freq', None, None, 'band')
- subspace: float32 [16, 2, 64, 64], P('freq')
The draws below stay inside these ranges and needn't reach their ends.
Inputs may be any that keep to these rules, and one draw needn't show every extreme that they name: `pair_index`: every pair number 0 to 1023 appears exactly once.
All inputs are finite; a program needn't handle non-finite values.
Results may differ from the reference program's by a relative error of at most 0.0085.
Values may be sent and summed in bfloat16 or wider, within the bound.
A program may use at most 128 MiB of HBM per device.

```python
import math
import jax
import jax.numpy as jnp
from jax import lax

NG = 8192
NV = 32
K = 64
NFREQ = 16
PAIRS = 1024
NC = 32


def block_scale(own_key, dims, shards, smallest, top_value):
    gain = 1.0
    for position, shards_of in shards:
        draws = jax.random.uniform(jax.random.fold_in(jax.random.fold_in(own_key, 6), position), (shards_of,), jnp.float32, smallest / len(shards), top_value / len(shards))
        gain = gain * jnp.repeat(jnp.exp(draws), dims[position] // shards_of).reshape((-1,) + (1,) * (len(dims) - 1 - position))
    return gain


def bell_draw(rng, extent, spread, most, shards=(), kind=jnp.bfloat16):
    loudness = block_scale(rng, extent, shards, -0.22, 0.18) if shards else 1.0
    array = jax.random.normal(rng, extent, jnp.float32) * spread * loudness
    return jnp.minimum(jnp.maximum(array, -most), most).astype(kind)


def setup_inputs(seed: int = 0) -> dict:
    keys = jax.random.split(jax.random.key(seed), 7)
    pair_density = bell_draw(keys[0], (PAIRS, 2, NG), 1.0, 6.0, ((0, 32),))
    trial_vectors = bell_draw(keys[1], (NFREQ, 2, K, NG), 1.0, 6.0, ((0, 4), (3, 8)))
    frequency = jnp.clip(jnp.exp(math.log(20.0) - 5.9914645 * jax.random.uniform(keys[2], (NFREQ,), jnp.float32) ** block_scale(keys[2], (NFREQ,), ((0, 4),), -0.2, 0.2)), 0.05, 20.0)
    val_energy = jnp.clip(jax.random.uniform(keys[3], (NV,), jnp.float32, -3.0, -0.1), -3.0, -0.1)
    cond_energy = jnp.clip(jax.random.uniform(keys[4], (NC,), jnp.float32, 0.1, 4.0), 0.1, 4.0)
    pair_index = jax.random.permutation(keys[5], PAIRS).astype(jnp.int32)
    return dict(pair_density=pair_density, trial_vectors=trial_vectors, frequency=frequency, val_energy=val_energy, cond_energy=cond_energy, pair_index=pair_index)


def pair_weights(pair_index, frequency, val_energy, cond_energy):
    delta = cond_energy[pair_index % NC] - val_energy[pair_index // NC]
    prefactor = 1.0 / math.sqrt(2.0 * NG * PAIRS)
    ratio = delta[None, :] / (delta[None, :] * delta[None, :] + frequency[:, None] * frequency[:, None])
    return (-4.0 * prefactor * ratio).astype(jnp.bfloat16)

def reference(pair_density, trial_vectors, frequency, val_energy, cond_energy, pair_index):
    density = pair_density.astype(jnp.float32)
    vectors = trial_vectors.astype(jnp.float32)
    weight = pair_weights(pair_index, frequency, val_energy, cond_energy).astype(jnp.float32)
    products = jnp.einsum('pcg,fekg->fcekp', density, vectors)
    over_real = products[:, 0, 0] + products[:, 1, 1]
    over_imag = products[:, 0, 1] - products[:, 1, 0]
    scaled_real = (weight[:, None, :] * over_real).astype(jnp.bfloat16)
    scaled_imag = (weight[:, None, :] * over_imag).astype(jnp.bfloat16)
    mixed = jnp.stack([jnp.stack([scaled_real, -scaled_imag], 1), jnp.stack([scaled_imag, scaled_real], 1)], 1)
    images = jnp.einsum('pcg,fdckp->fdkg', density, mixed.astype(jnp.float32))
    hp = lax.Precision.HIGHEST
    real_part = jnp.einsum('fkg,flg->fkl', vectors[:, 0], images[:, 0], precision=hp) + jnp.einsum('fkg,flg->fkl', vectors[:, 1], images[:, 1], precision=hp)
    imag_part = jnp.einsum('fkg,flg->fkl', vectors[:, 0], images[:, 1], precision=hp) - jnp.einsum('fkg,flg->fkl', vectors[:, 1], images[:, 0], precision=hp)
    subspace = jnp.stack([real_part, imag_part], 1) / NG
    return (images, subspace)
```

```python
import functools
import math

import jax
import jax.numpy as jnp
from jax import lax
from jax.experimental import pallas as pl
from jax.experimental.pallas import tpu as pltpu
from jax.sharding import PartitionSpec as P

MESH = pl.DeviceIdType.MESH
F32 = jnp.float32
BF16 = jnp.bfloat16


def local_delta(pair_index, val_energy, cond_energy):
    cond_count = cond_energy.shape[0]
    val_count = val_energy.shape[0]
    cond_pick = jnp.sum(
        jnp.where(
            (pair_index % cond_count)[:, None] == jnp.arange(cond_count)[None, :],
            cond_energy[None, :],
            0.0,
        ),
        axis=1,
    )
    val_pick = jnp.sum(
        jnp.where(
            (pair_index // cond_count)[:, None] == jnp.arange(val_count)[None, :],
            val_energy[None, :],
            0.0,
        ),
        axis=1,
    )
    return cond_pick - val_pick


def kernel(
    groups, members, freqs, vecs, rows, grid_here, prefactor, inv_grid,
    dens, trial, freq_row, delta_own,
    images, sub,
    held, mix, deltas, part_out, part_in, own, ring_out, ring_in, scaled, acc,
    sem_as, sem_ar, sem_fs, sem_fr, sem_ds, sem_dr, sem_es, sem_er,
    sem_ps, sem_pr, sem_rs, sem_rr, sem_gs, sem_gr, sem_hs, sem_hr,
):
    f = lax.axis_index("freq")
    b = lax.axis_index("band")
    chips = members // 2
    chunks = members // 2
    zc = b // 2
    core = b % 2
    width = freqs * 2 * vecs
    chunk_rows = 2 * groups * rows
    partner = zc * 2 + (1 - core)

    def remote(src, dst, send, recv, freq_id, band_id):
        return pltpu.make_async_remote_copy(
            src_ref=src, dst_ref=dst, send_sem=send, recv_sem=recv,
            device_id=(freq_id, band_id), device_id_type=MESH,
        )

    barrier = pltpu.get_barrier_semaphore()
    for s in range(1, members):
        pl.semaphore_signal(barrier, inc=1, device_id=(f, (b + s) % members), device_id_type=MESH)
    for s in range(1, groups):
        pl.semaphore_signal(barrier, inc=1, device_id=((f + s) % groups, b), device_id_type=MESH)
    pl.semaphore_wait(barrier, members + groups - 2)

    sends = []

    def go(copy):
        copy.start()
        sends.append(copy)

    mine = pltpu.make_async_copy(dens.at[b], held.at[b, f], sem_ar.at[b])
    mine.start()
    for s in range(1, members):
        to = (b + s) % members
        go(remote(dens.at[to], held.at[b, f], sem_as.at[s], sem_ar.at[b], f, to))
    mine_delta = pltpu.make_async_copy(delta_own, deltas.at[f, b], sem_dr.at[b])
    mine_delta.start()
    for s in range(1, members):
        to = (b + s) % members
        go(remote(delta_own, deltas.at[f, b], sem_ds.at[s], sem_dr.at[b], f, to))

    for q in range(freqs):
        lo, hi = q * 2 * vecs, (q * 2 + 1) * vecs
        top = trial[lo : lo + vecs, :]
        low = trial[hi : hi + vecs, :]
        mix[lo : lo + vecs, 0:grid_here] = top
        mix[lo : lo + vecs, grid_here:] = low
        mix[hi : hi + vecs, 0:grid_here] = low
        mix[hi : hi + vecs, grid_here:] = -top

    for j in range(members):
        pltpu.make_async_copy(delta_own, deltas.at[f, j], sem_dr.at[j]).wait()
    for s in range(1, groups):
        go(remote(deltas.at[f], deltas.at[f], sem_es.at[s], sem_er.at[s], (f + s) % groups, b))

    for j in range(members):
        pltpu.make_async_copy(dens.at[0], held.at[j, f], sem_ar.at[j]).wait()
        for s in range(1, groups):
            go(remote(held.at[j, f], held.at[j, f], sem_fs.at[j, s], sem_fr.at[j, s], (f + s) % groups, b))

    for s in range(1, groups):
        src = (f + groups - s) % groups
        remote(deltas.at[src], deltas.at[src], sem_es.at[s], sem_er.at[s], src, b).wait_recv()

    def weights(column):
        ratio = column / (column * column + freq_row[...] * freq_row[...])
        return (-4.0 * prefactor * ratio).astype(BF16).astype(F32)

    def block_delta(g, j):
        return jnp.transpose(deltas[g, j])[0:rows, 0:1]

    def cross(j):
        for m in (2 * j, 2 * j + 1):
            for s in range(1, groups):
                src = (f + groups - s) % groups
                remote(held.at[m, src], held.at[m, src], sem_fs.at[m, s], sem_fr.at[m, s], src, b).wait_recv()
        block = held[2 * j : 2 * j + 2].reshape(chunk_rows, 2 * grid_here)
        own[...] = lax.dot_general(
            block, mix[...], (((1,), (1,)), ((), ())), preferred_element_type=F32
        ).reshape(2, chips, chunk_rows // members, width)
        part_out[j] = own[1 - core].astype(BF16)
        go(remote(part_out.at[j], part_in.at[j], sem_ps.at[j], sem_pr.at[j], f, partner))
        remote(part_out.at[j], part_in.at[j], sem_ps.at[j], sem_pr.at[j], f, partner).wait_recv()
        total = own[core] + part_in[j].astype(F32)
        ring_out[j] = total.astype(BF16)
        for s in range(1, chips):
            to = (zc + s) % chips
            go(remote(ring_out.at[j, to], ring_in.at[j, s], sem_rs.at[j, s], sem_rr.at[j, s], f, to * 2 + core))

    def scale(j):
        total = ring_out[j, zc].astype(F32)
        for s in range(1, chips):
            src = (zc + chips - s) % chips
            remote(ring_out.at[j, zc], ring_in.at[j, s], sem_rs.at[j, s], sem_rr.at[j, s], f, src * 2 + core).wait_recv()
            total = total + ring_in[j, s].astype(F32)
        q = core * chips + zc
        column = block_delta(q % groups, 2 * j + q // groups)
        scaled[j, core, zc] = (weights(column) * total).astype(BF16)
        for s in range(1, chips):
            to = (zc + s) % chips
            go(remote(scaled.at[j, core, zc], scaled.at[j, core, zc], sem_gs.at[j, s], sem_gr.at[j, s], f, to * 2 + core))

    def share(j):
        for s in range(1, chips):
            src = (zc + chips - s) % chips
            remote(scaled.at[j, core, src], scaled.at[j, core, src], sem_gs.at[j, s], sem_gr.at[j, s], f, src * 2 + core).wait_recv()
        go(remote(scaled.at[j, core], scaled.at[j, core], sem_hs.at[j], sem_hr.at[j], f, partner))

    def image(j):
        remote(scaled.at[j, 1 - core], scaled.at[j, 1 - core], sem_hs.at[j], sem_hr.at[j], f, partner).wait_recv()
        flat = scaled[j].reshape(chunk_rows, width)
        flat32 = flat.astype(F32)
        lane = lax.broadcasted_iota(jnp.int32, (1, 2 * vecs), 1)
        sign = jnp.where(lane < vecs, -1.0, 1.0)
        turned = jnp.concatenate(
            [
                pltpu.roll(flat32[:, q * 2 * vecs : (q + 1) * 2 * vecs], vecs, 1) * sign
                for q in range(freqs)
            ],
            axis=1,
        ).astype(BF16)
        over_rows = (((0,), (0,)), ((), ()))
        real = held[2 * j : 2 * j + 2, :, :, 0:grid_here].reshape(chunk_rows, grid_here)
        imag = held[2 * j : 2 * j + 2, :, :, grid_here:].reshape(chunk_rows, grid_here)
        term = lax.dot_general(flat, real, over_rows, preferred_element_type=F32) + lax.dot_general(
            turned, imag, over_rows, preferred_element_type=F32
        )
        column = jnp.concatenate(
            [block_delta(q % groups, 2 * j + q // groups) for q in range(2 * groups)], axis=0
        )
        crossing = (flat32 / weights(column)).astype(BF16)
        for q in range(freqs):
            lo, hi = q * 2 * vecs, (q + 1) * 2 * vecs
            square = lax.dot_general(
                crossing[:, lo:hi], flat[:, lo:hi], over_rows, preferred_element_type=F32
            )
            if j == 0:
                acc[q] = square
            else:
                acc[q] = acc[q] + square
        if j == 0:
            images[...] = term
        else:
            images[...] = images[...] + term

    for t in range(chunks + 2):
        if t < chunks:
            cross(t)
        if 0 <= t - 1 < chunks:
            scale(t - 1)
        if 0 <= t - 2 < chunks:
            share(t - 2)
            image(t - 2)

    for q in range(freqs):
        square = acc[q]
        lo, hi = q * 2 * vecs, (q * 2 + 1) * vecs
        sub[lo : lo + vecs, :] = (square[0:vecs, 0:vecs] + square[vecs:, vecs:]) * inv_grid
        sub[hi : hi + vecs, :] = (square[0:vecs, vecs:] - square[vecs:, 0:vecs]) * inv_grid

    for copy in sends:
        copy.wait_send()


def shards(pair_density, trial_vectors, frequency, val_energy, cond_energy, pair_index):
    groups = lax.axis_size("freq")
    members = lax.axis_size("band")
    rows = pair_density.shape[0]
    freqs, _, vecs, grid_here = trial_vectors.shape
    pair_count = rows * groups * members
    grid_count = grid_here * members
    prefactor = 1.0 / math.sqrt(2.0 * grid_count * pair_count)
    width = freqs * 2 * vecs
    chips = members // 2
    chunks = members // 2
    slot = 2 * groups * rows // members
    dens = jnp.transpose(
        pair_density.reshape(rows, 2, members, grid_here), (2, 0, 1, 3)
    ).reshape(members, rows, 2 * grid_here)
    trial = trial_vectors.reshape(width, grid_here)
    freq_row = jnp.repeat(frequency, 2 * vecs)[None, :]
    delta = local_delta(pair_index, val_energy, cond_energy)
    delta_own = jnp.broadcast_to(jnp.pad(delta, (0, 128 - rows))[None, :], (8, 128))
    dma = pltpu.SemaphoreType.DMA
    vmem = pl.BlockSpec(memory_space=pltpu.VMEM)
    images, sub = pl.pallas_call(
        functools.partial(
            kernel, groups, members, freqs, vecs, rows, grid_here, prefactor, 1.0 / grid_count
        ),
        out_shape=(
            jax.ShapeDtypeStruct((width, grid_here), F32),
            jax.ShapeDtypeStruct((width, vecs), F32),
        ),
        in_specs=[vmem] * 4,
        out_specs=(vmem, vmem),
        scratch_shapes=[
            pltpu.VMEM((members, groups, rows, 2 * grid_here), BF16),
            pltpu.VMEM((width, 2 * grid_here), BF16),
            pltpu.VMEM((groups, members, 8, 128), F32),
            pltpu.VMEM((chunks, chips, slot, width), BF16),
            pltpu.VMEM((chunks, chips, slot, width), BF16),
            pltpu.VMEM((2, chips, slot, width), F32),
            pltpu.VMEM((chunks, chips, slot, width), BF16),
            pltpu.VMEM((chunks, chips, slot, width), BF16),
            pltpu.VMEM((chunks, 2, chips, slot, width), BF16),
            pltpu.VMEM((freqs, 2 * vecs, 2 * vecs), F32),
            dma((members,)), dma((members,)),
            dma((members, groups)), dma((members, groups)),
            dma((members,)), dma((members,)),
            dma((groups,)), dma((groups,)),
            dma((chunks,)), dma((chunks,)),
            dma((chunks, chips)), dma((chunks, chips)),
            dma((chunks, chips)), dma((chunks, chips)),
            dma((chunks,)), dma((chunks,)),
        ],
        compiler_params=pltpu.CompilerParams(
            collective_id=0, has_side_effects=True, vmem_limit_bytes=56 * 1024 * 1024
        ),
    )(dens, trial, freq_row, delta_own)
    return (
        images.reshape(freqs, 2, vecs, grid_here),
        sub.reshape(freqs, 2, vecs, vecs),
    )


def solution(mesh):
    return jax.shard_map(
        shards,
        mesh=mesh,
        in_specs=(
            P(("freq", "band"), None, None),
            P("freq", None, None, "band"),
            P("freq"),
            P(),
            P(),
            P(("freq", "band")),
        ),
        out_specs=(P("freq", None, None, "band"), P("freq", None, None, None)),
        check_vma=False,
    )
```

```python
import functools
import math

import jax
import jax.numpy as jnp
from jax import lax
from jax.experimental import pallas as pl
from jax.experimental.pallas import tpu as pltpu
from jax.sharding import PartitionSpec as P

MESH = pl.DeviceIdType.MESH
F32 = jnp.float32
BF16 = jnp.bfloat16


def local_delta(pair_index, val_energy, cond_energy):
    cond_count = cond_energy.shape[0]
    val_count = val_energy.shape[0]
    cond_pick = jnp.sum(
        jnp.where(
            (pair_index % cond_count)[:, None] == jnp.arange(cond_count)[None, :],
            cond_energy[None, :],
            0.0,
        ),
        axis=1,
    )
    val_pick = jnp.sum(
        jnp.where(
            (pair_index // cond_count)[:, None] == jnp.arange(val_count)[None, :],
            val_energy[None, :],
            0.0,
        ),
        axis=1,
    )
    return cond_pick - val_pick


def kernel(
    groups, members, chunks, freqs, vecs, rows, grid_here, prefactor, inv_grid,
    dens, trial, freq_row, delta_own,
    images, sub,
    held, mix, deltas, cols, part_out, part_in, own, ring_out, ring_in, scaled, acc,
    sem_as, sem_ar, sem_fs, sem_fr, sem_ds, sem_dr, sem_es, sem_er,
    sem_ps, sem_pr, sem_rs, sem_rr, sem_gs, sem_gr, sem_hs, sem_hr,
):
    f = lax.axis_index("freq")
    b = lax.axis_index("band")
    chips = members // 2
    piece = rows // chunks
    zc = b // 2
    core = b % 2
    width = freqs * 2 * vecs
    chunk_rows = groups * members * piece
    slot = groups * piece
    partner = zc * 2 + (1 - core)

    def remote(src, dst, send, recv, freq_id, band_id):
        return pltpu.make_async_remote_copy(
            src_ref=src, dst_ref=dst, send_sem=send, recv_sem=recv,
            device_id=(freq_id, band_id), device_id_type=MESH,
        )

    barrier = pltpu.get_barrier_semaphore()
    for s in range(1, members):
        pl.semaphore_signal(barrier, inc=1, device_id=(f, (b + s) % members), device_id_type=MESH)
    for s in range(1, groups):
        pl.semaphore_signal(barrier, inc=1, device_id=((f + s) % groups, b), device_id_type=MESH)
    pl.semaphore_wait(barrier, members + groups - 2)

    sends = []

    def go(copy):
        copy.start()
        sends.append(copy)

    for c in range(chunks):
        pltpu.make_async_copy(dens.at[c, b], held.at[c, f, b], sem_ar.at[c, b]).start()
        for s in range(1, members):
            to = (b + s) % members
            go(remote(dens.at[c, to], held.at[c, f, b], sem_as.at[c, s], sem_ar.at[c, b], f, to))
        if c == 0:
            mine_delta = pltpu.make_async_copy(delta_own, deltas.at[f, b], sem_dr.at[b])
            mine_delta.start()
            for s in range(1, members):
                to = (b + s) % members
                go(remote(delta_own, deltas.at[f, b], sem_ds.at[s], sem_dr.at[b], f, to))

    for q in range(freqs):
        lo, hi = q * 2 * vecs, (q * 2 + 1) * vecs
        top = trial[lo : lo + vecs, :]
        low = trial[hi : hi + vecs, :]
        mix[lo : lo + vecs, 0:grid_here] = top
        mix[lo : lo + vecs, grid_here:] = low
        mix[hi : hi + vecs, 0:grid_here] = low
        mix[hi : hi + vecs, grid_here:] = -top

    for j in range(members):
        pltpu.make_async_copy(delta_own, deltas.at[f, j], sem_dr.at[j]).wait()
    for s in range(1, groups):
        go(remote(deltas.at[f], deltas.at[f], sem_es.at[s], sem_er.at[s], (f + s) % groups, b))

    square_groups = groups == 4
    xx, yy = f % 2, f // 2
    fx, fy = yy * 2 + (1 - xx), (1 - yy) * 2 + xx
    fd = (1 - yy) * 2 + (1 - xx)
    half = members // 2

    def whole(c, g, lane, peer):
        return remote(held.at[c, g], held.at[c, g], sem_fs.at[c, lane], sem_fr.at[c, lane], peer, b)

    def part(c, g, first, lane, peer):
        ref = held.at[c, g, first : first + half]
        return remote(ref, ref, sem_fs.at[c, lane], sem_fr.at[c, lane], peer, b)

    def spread(c):
        for j in range(members):
            pltpu.make_async_copy(dens.at[c, 0], held.at[c, f, j], sem_ar.at[c, j]).wait()
        if square_groups:
            go(whole(c, f, 0, fx))
            go(whole(c, f, 1, fy))
        else:
            for s in range(1, groups):
                go(whole(c, f, s, (f + s) % groups))

    def relay(c):
        if square_groups:
            whole(c, fx, 0, fx).wait_recv()
            go(part(c, fx, 0, 2, fy))
            whole(c, fy, 1, fy).wait_recv()
            go(part(c, fy, half, 3, fx))

    def arrive(c):
        if square_groups:
            part(c, fd, 0, 2, fy).wait_recv()
            part(c, fd, half, 3, fx).wait_recv()
        else:
            for s in range(1, groups):
                src = (f + groups - s) % groups
                whole(c, src, s, src).wait_recv()

    def columns():
        for s in range(1, groups):
            src = (f + groups - s) % groups
            remote(deltas.at[src], deltas.at[src], sem_es.at[s], sem_er.at[s], src, b).wait_recv()
        for g in range(groups):
            for j in range(members):
                turned = jnp.transpose(deltas[g, j])
                at = (g * members + j) * piece
                for c in range(chunks):
                    cols[c, at : at + piece, :] = turned[c * piece : (c + 1) * piece, :]

    def weights(column):
        ratio = column / (column * column + freq_row[...] * freq_row[...])
        return (-4.0 * prefactor * ratio).astype(BF16).astype(F32)

    def cross(j):
        arrive(j)
        block = held[j].reshape(chunk_rows, 2 * grid_here)
        own[...] = lax.dot_general(
            block, mix[...], (((1,), (1,)), ((), ())), preferred_element_type=F32
        ).reshape(2, chips, chunk_rows // members, width)
        part_out[j] = own[1 - core].astype(BF16)
        go(remote(part_out.at[j], part_in.at[j], sem_ps.at[j], sem_pr.at[j], f, partner))
        remote(part_out.at[j], part_in.at[j], sem_ps.at[j], sem_pr.at[j], f, partner).wait_recv()
        total = own[core] + part_in[j].astype(F32)
        ring_out[j] = total.astype(BF16)
        for s in range(1, chips):
            to = (zc + s) % chips
            go(remote(ring_out.at[j, to], ring_in.at[j, s], sem_rs.at[j, s], sem_rr.at[j, s], f, to * 2 + core))

    def scale(j):
        total = ring_out[j, zc].astype(F32)
        for s in range(1, chips):
            src = (zc + chips - s) % chips
            remote(ring_out.at[j, zc], ring_in.at[j, s], sem_rs.at[j, s], sem_rr.at[j, s], f, src * 2 + core).wait_recv()
            total = total + ring_in[j, s].astype(F32)
        q = core * chips + zc
        column = cols[j, pl.ds(pl.multiple_of(q * slot, 8), slot), 0:1]
        scaled[j, core, zc] = (weights(column) * total).astype(BF16)
        for s in range(1, chips):
            to = (zc + s) % chips
            go(remote(scaled.at[j, core, zc], scaled.at[j, core, zc], sem_gs.at[j, s], sem_gr.at[j, s], f, to * 2 + core))

    def share(j):
        for s in range(1, chips):
            src = (zc + chips - s) % chips
            remote(scaled.at[j, core, src], scaled.at[j, core, src], sem_gs.at[j, s], sem_gr.at[j, s], f, src * 2 + core).wait_recv()
        go(remote(scaled.at[j, core], scaled.at[j, core], sem_hs.at[j], sem_hr.at[j], f, partner))

    def image(j):
        remote(scaled.at[j, 1 - core], scaled.at[j, 1 - core], sem_hs.at[j], sem_hr.at[j], f, partner).wait_recv()
        flat = scaled[j].reshape(chunk_rows, width)
        flat32 = flat.astype(F32)
        lane = lax.broadcasted_iota(jnp.int32, (1, 2 * vecs), 1)
        sign = jnp.where(lane < vecs, -1.0, 1.0)
        turned = jnp.concatenate(
            [
                pltpu.roll(flat32[:, q * 2 * vecs : (q + 1) * 2 * vecs], vecs, 1) * sign
                for q in range(freqs)
            ],
            axis=1,
        ).astype(BF16)
        over_rows = (((0,), (0,)), ((), ()))
        real = held[j, :, :, :, 0:grid_here].reshape(chunk_rows, grid_here)
        imag = held[j, :, :, :, grid_here:].reshape(chunk_rows, grid_here)
        term = lax.dot_general(flat, real, over_rows, preferred_element_type=F32) + lax.dot_general(
            turned, imag, over_rows, preferred_element_type=F32
        )
        column = cols[j, :, 0:1]
        crossing = (flat32 / weights(column)).astype(BF16)
        for q in range(freqs):
            lo, hi = q * 2 * vecs, (q + 1) * 2 * vecs
            square = lax.dot_general(
                crossing[:, lo:hi], flat[:, lo:hi], over_rows, preferred_element_type=F32
            )
            if j == 0:
                acc[q] = square
            else:
                acc[q] = acc[q] + square
        if j == 0:
            images[...] = term
        else:
            images[...] = images[...] + term

    spread(0)
    columns()
    for t in range(chunks + 2):
        if t + 1 < chunks:
            spread(t + 1)
        if t < chunks:
            relay(t)
            cross(t)
        if 0 <= t - 1 < chunks:
            scale(t - 1)
        if 0 <= t - 2 < chunks:
            share(t - 2)
            image(t - 2)

    for q in range(freqs):
        square = acc[q]
        lo, hi = q * 2 * vecs, (q * 2 + 1) * vecs
        sub[lo : lo + vecs, :] = (square[0:vecs, 0:vecs] + square[vecs:, vecs:]) * inv_grid
        sub[hi : hi + vecs, :] = (square[0:vecs, vecs:] - square[vecs:, 0:vecs]) * inv_grid

    for copy in sends:
        copy.wait_send()


def shards(pair_density, trial_vectors, frequency, val_energy, cond_energy, pair_index):
    groups = lax.axis_size("freq")
    members = lax.axis_size("band")
    rows = pair_density.shape[0]
    freqs, _, vecs, grid_here = trial_vectors.shape
    pair_count = rows * groups * members
    grid_count = grid_here * members
    prefactor = 1.0 / math.sqrt(2.0 * grid_count * pair_count)
    width = freqs * 2 * vecs
    chips = members // 2
    chunks = rows // 8
    piece = rows // chunks
    slot = groups * piece
    dens = jnp.transpose(
        pair_density.reshape(chunks, piece, 2, members, grid_here), (0, 3, 1, 2, 4)
    ).reshape(chunks, members, piece, 2 * grid_here)
    trial = trial_vectors.reshape(width, grid_here)
    freq_row = jnp.repeat(frequency, 2 * vecs)[None, :]
    delta = local_delta(pair_index, val_energy, cond_energy)
    delta_own = jnp.broadcast_to(jnp.pad(delta, (0, 128 - rows))[None, :], (8, 128))
    dma = pltpu.SemaphoreType.DMA
    vmem = pl.BlockSpec(memory_space=pltpu.VMEM)
    images, sub = pl.pallas_call(
        functools.partial(
            kernel, groups, members, chunks, freqs, vecs, rows, grid_here, prefactor, 1.0 / grid_count
        ),
        out_shape=(
            jax.ShapeDtypeStruct((width, grid_here), F32),
            jax.ShapeDtypeStruct((width, vecs), F32),
        ),
        in_specs=[vmem] * 4,
        out_specs=(vmem, vmem),
        scratch_shapes=[
            pltpu.VMEM((chunks, groups, members, piece, 2 * grid_here), BF16),
            pltpu.VMEM((width, 2 * grid_here), BF16),
            pltpu.VMEM((groups, members, 8, 128), F32),
            pltpu.VMEM((chunks, members * slot, 8), F32),
            pltpu.VMEM((chunks, chips, slot, width), BF16),
            pltpu.VMEM((chunks, chips, slot, width), BF16),
            pltpu.VMEM((2, chips, slot, width), F32),
            pltpu.VMEM((chunks, chips, slot, width), BF16),
            pltpu.VMEM((chunks, chips, slot, width), BF16),
            pltpu.VMEM((chunks, 2, chips, slot, width), BF16),
            pltpu.VMEM((freqs, 2 * vecs, 2 * vecs), F32),
            dma((chunks, members)), dma((chunks, members)),
            dma((chunks, groups)), dma((chunks, groups)),
            dma((members,)), dma((members,)),
            dma((groups,)), dma((groups,)),
            dma((chunks,)), dma((chunks,)),
            dma((chunks, chips)), dma((chunks, chips)),
            dma((chunks, chips)), dma((chunks, chips)),
            dma((chunks,)), dma((chunks,)),
        ],
        compiler_params=pltpu.CompilerParams(
            collective_id=0, has_side_effects=True, vmem_limit_bytes=56 * 1024 * 1024
        ),
    )(dens, trial, freq_row, delta_own)
    return (
        images.reshape(freqs, 2, vecs, grid_here),
        sub.reshape(freqs, 2, vecs, vecs),
    )


def solution(mesh):
    return jax.shard_map(
        shards,
        mesh=mesh,
        in_specs=(
            P(("freq", "band"), None, None),
            P("freq", None, None, "band"),
            P("freq"),
            P(),
            P(),
            P(("freq", "band")),
        ),
        out_specs=(P("freq", None, None, "band"), P("freq", None, None, None)),
        check_vma=False,
    )
```

```python
import functools
import math

import jax
import jax.numpy as jnp
from jax import lax
from jax.experimental import pallas as pl
from jax.experimental.pallas import tpu as pltpu
from jax.sharding import PartitionSpec as P

MESH = pl.DeviceIdType.MESH
F32 = jnp.float32
BF16 = jnp.bfloat16


def kernel(
    groups, members, chunks, freqs, vecs, rows, grid_here, prefactor, inv_grid,
    dens, trial, frequency, val_energy, cond_energy, pair_index,
    images, sub,
    held, mix, delta_own, freq_row, deltas, cols, part_out, part_in, own, ring_out, ring_in, scaled, acc,
    sem_as, sem_ar, sem_fs, sem_fr, sem_ds, sem_dr, sem_es, sem_er,
    sem_ps, sem_pr, sem_rs, sem_rr, sem_gs, sem_gr, sem_hs, sem_hr,
):
    f = lax.axis_index("freq")
    b = lax.axis_index("band")
    chips = members // 2
    piece = rows // chunks
    zc = b // 2
    core = b % 2
    width = freqs * 2 * vecs
    chunk_rows = groups * members * piece
    slot = groups * piece
    partner = zc * 2 + (1 - core)

    def remote(src, dst, send, recv, freq_id, band_id):
        return pltpu.make_async_remote_copy(
            src_ref=src, dst_ref=dst, send_sem=send, recv_sem=recv,
            device_id=(freq_id, band_id), device_id_type=MESH,
        )

    barrier = pltpu.get_barrier_semaphore()
    for s in range(1, members):
        pl.semaphore_signal(barrier, inc=1, device_id=(f, (b + s) % members), device_id_type=MESH)
    for s in range(1, groups):
        pl.semaphore_signal(barrier, inc=1, device_id=((f + s) % groups, b), device_id_type=MESH)
    pl.semaphore_wait(barrier, members + groups - 2)

    sends = []

    def go(copy):
        copy.start()
        sends.append(copy)

    for c in range(chunks):
        pltpu.make_async_copy(dens.at[c, b], held.at[c, f, b], sem_ar.at[c, b]).start()
        go(remote(dens.at[c, partner], held.at[c, f, b], sem_as.at[c, 0], sem_ar.at[c, b], f, partner))
    def exchange(c):
        for r in range(1, chips):
            for k in range(2):
                to = (zc + r) % chips * 2 + (core + k) % 2
                go(remote(dens.at[c, to], held.at[c, f, b], sem_as.at[c, 2 * r + k], sem_ar.at[c, b], f, to))

    cond_count = cond_energy.shape[0]
    val_count = val_energy.shape[0]
    index = pair_index[...]
    rest_index = index
    val_pick = jnp.full(index.shape, val_energy[0], F32)
    for v in range(1, val_count):
        above = index >= v * cond_count
        val_pick = jnp.where(above, val_energy[v], val_pick)
        rest_index = jnp.where(above, index - v * cond_count, rest_index)
    cond_pick = jnp.full(index.shape, cond_energy[0], F32)
    for v in range(1, cond_count):
        cond_pick = jnp.where(rest_index == v, cond_energy[v], cond_pick)
    delta_own[...] = jnp.ones_like(delta_own)
    delta_own[0:1, 0:rows] = cond_pick - val_pick
    for q in range(freqs):
        freq_row[:, q * 2 * vecs : (q + 1) * 2 * vecs] = jnp.full((1, 2 * vecs), frequency[q], F32)
    pltpu.make_async_copy(delta_own, deltas.at[f, b], sem_dr.at[b]).start()
    for s in range(1, members):
        to = (b + s) % members
        go(remote(delta_own, deltas.at[f, b], sem_ds.at[s], sem_dr.at[b], f, to))

    for q in range(freqs):
        lo, hi = q * 2 * vecs, (q * 2 + 1) * vecs
        top = trial[lo : lo + vecs, :]
        low = trial[hi : hi + vecs, :]
        mix[lo : lo + vecs, 0:grid_here] = top
        mix[lo : lo + vecs, grid_here:] = low
        mix[hi : hi + vecs, 0:grid_here] = low
        mix[hi : hi + vecs, grid_here:] = -top

    square_groups = groups == 4
    xx, yy = f % 2, f // 2
    fx, fy = yy * 2 + (1 - xx), (1 - yy) * 2 + xx
    fd = (1 - yy) * 2 + (1 - xx)

    def piece_copy(c, g, z, lane, peer):
        ref = held.at[c, g, pl.ds(2 * z, 2)]
        return remote(ref, ref, sem_fs.at[c, lane, z], sem_fr.at[c, lane, z], peer, b)

    def whole(c, g, lane, peer):
        return remote(held.at[c, g], held.at[c, g], sem_fs.at[c, lane, 0], sem_fr.at[c, lane, 0], peer, b)

    def spread(c, offsets):
        for r in offsets:
            z = (zc + r) % chips
            for k in range(2):
                j = z * 2 + k
                pltpu.make_async_copy(dens.at[c, 0], held.at[c, f, j], sem_ar.at[c, j]).wait()
            if square_groups:
                go(piece_copy(c, f, z, 0, fx))
                go(piece_copy(c, f, z, 1, fy))
        if not square_groups and offsets[-1] == chips - 1:
            for s in range(1, groups):
                go(whole(c, f, s, (f + s) % groups))

    def relay(c):
        if square_groups:
            for r in range(chips):
                z = (zc + r) % chips
                if r % 2 == 0:
                    piece_copy(c, fx, z, 0, fx).wait_recv()
                    go(piece_copy(c, fx, z, 2, fy))
                else:
                    piece_copy(c, fy, z, 1, fy).wait_recv()
                    go(piece_copy(c, fy, z, 3, fx))

    def arrive(c):
        if square_groups:
            for r in range(chips):
                z = (zc + r) % chips
                if r % 2 == 0:
                    piece_copy(c, fy, z, 1, fy).wait_recv()
                    piece_copy(c, fd, z, 2, fy).wait_recv()
                else:
                    piece_copy(c, fx, z, 0, fx).wait_recv()
                    piece_copy(c, fd, z, 3, fx).wait_recv()
        else:
            for s in range(1, groups):
                src = (f + groups - s) % groups
                whole(c, src, s, src).wait_recv()

    def pass_deltas():
        for j in range(members):
            pltpu.make_async_copy(delta_own, deltas.at[f, j], sem_dr.at[j]).wait()
        for s in range(1, groups):
            go(remote(deltas.at[f], deltas.at[f], sem_es.at[s], sem_er.at[s], (f + s) % groups, b))

    def columns():
        for s in range(1, groups):
            src = (f + groups - s) % groups
            remote(deltas.at[src], deltas.at[src], sem_es.at[s], sem_er.at[s], src, b).wait_recv()
        for g in range(groups):
            for j in range(members):
                turned = jnp.transpose(deltas[g, j])
                at = (g * members + j) * piece
                for c in range(chunks):
                    cols[c, at : at + piece, :] = turned[c * piece : (c + 1) * piece, :]

    def weights(column):
        ratio = column / (column * column + freq_row[...] * freq_row[...])
        return (-4.0 * prefactor * ratio).astype(BF16).astype(F32)

    def cross(j):
        arrive(j)
        block = held[j].reshape(chunk_rows, 2 * grid_here)
        own[...] = lax.dot_general(
            block, mix[...], (((1,), (1,)), ((), ())), preferred_element_type=F32
        ).reshape(2, chips, chunk_rows // members, width)
        part_out[j] = own[1 - core].astype(BF16)
        go(remote(part_out.at[j], part_in.at[j], sem_ps.at[j], sem_pr.at[j], f, partner))
        remote(part_out.at[j], part_in.at[j], sem_ps.at[j], sem_pr.at[j], f, partner).wait_recv()
        total = own[core] + part_in[j].astype(F32)
        ring_out[j] = total.astype(BF16)
        for s in range(1, chips):
            to = (zc + s) % chips
            go(remote(ring_out.at[j, to], ring_in.at[j, s], sem_rs.at[j, s], sem_rr.at[j, s], f, to * 2 + core))

    def scale(j):
        total = ring_out[j, zc].astype(F32)
        for s in range(1, chips):
            src = (zc + chips - s) % chips
            remote(ring_out.at[j, zc], ring_in.at[j, s], sem_rs.at[j, s], sem_rr.at[j, s], f, src * 2 + core).wait_recv()
            total = total + ring_in[j, s].astype(F32)
        q = core * chips + zc
        column = cols[j, pl.ds(pl.multiple_of(q * slot, 8), slot), 0:1]
        scaled[j, core, zc] = (weights(column) * total).astype(BF16)
        for s in range(1, chips):
            to = (zc + s) % chips
            go(remote(scaled.at[j, core, zc], scaled.at[j, core, zc], sem_gs.at[j, s], sem_gr.at[j, s], f, to * 2 + core))

    def share(j):
        for s in range(1, chips):
            src = (zc + chips - s) % chips
            remote(scaled.at[j, core, src], scaled.at[j, core, src], sem_gs.at[j, s], sem_gr.at[j, s], f, src * 2 + core).wait_recv()
        go(remote(scaled.at[j, core], scaled.at[j, core], sem_hs.at[j], sem_hr.at[j], f, partner))

    def image(j):
        remote(scaled.at[j, 1 - core], scaled.at[j, 1 - core], sem_hs.at[j], sem_hr.at[j], f, partner).wait_recv()
        flat = scaled[j].reshape(chunk_rows, width)
        flat32 = flat.astype(F32)
        lane = lax.broadcasted_iota(jnp.int32, (1, 2 * vecs), 1)
        sign = jnp.where(lane < vecs, -1.0, 1.0)
        turned = jnp.concatenate(
            [
                pltpu.roll(flat32[:, q * 2 * vecs : (q + 1) * 2 * vecs], vecs, 1) * sign
                for q in range(freqs)
            ],
            axis=1,
        ).astype(BF16)
        over_rows = (((0,), (0,)), ((), ()))
        real = held[j, :, :, :, 0:grid_here].reshape(chunk_rows, grid_here)
        imag = held[j, :, :, :, grid_here:].reshape(chunk_rows, grid_here)
        term = lax.dot_general(flat, real, over_rows, preferred_element_type=F32) + lax.dot_general(
            turned, imag, over_rows, preferred_element_type=F32
        )
        column = cols[j, :, 0:1]
        crossing = (flat32 / weights(column)).astype(BF16)
        for q in range(freqs):
            lo, hi = q * 2 * vecs, (q + 1) * 2 * vecs
            square = lax.dot_general(
                crossing[:, lo:hi], flat[:, lo:hi], over_rows, preferred_element_type=F32
            )
            if j == 0:
                acc[q] = square
            else:
                acc[q] = acc[q] + square
        if j == 0:
            images[...] = term
        else:
            images[...] = images[...] + term

    exchange(0)
    for c in range(chunks):
        spread(c, (0,))
    exchange(1)
    pass_deltas()
    for t in range(chunks + 4):
        if t < chunks:
            spread(t, range(1, chips))
        if t + 2 < chunks:
            exchange(t + 2)
        if t == 0:
            columns()
        if 0 <= t - 1 < chunks:
            relay(t - 1)
        if 0 <= t - 3 < chunks:
            scale(t - 3)
        if 0 <= t - 2 < chunks:
            cross(t - 2)
        if 0 <= t - 4 < chunks:
            share(t - 4)
            image(t - 4)

    for q in range(freqs):
        square = acc[q]
        lo, hi = q * 2 * vecs, (q * 2 + 1) * vecs
        sub[lo : lo + vecs, :] = (square[0:vecs, 0:vecs] + square[vecs:, vecs:]) * inv_grid
        sub[hi : hi + vecs, :] = (square[0:vecs, vecs:] - square[vecs:, 0:vecs]) * inv_grid

    for copy in sends:
        copy.wait_send()


def shards(pair_density, trial_vectors, frequency, val_energy, cond_energy, pair_index):
    groups = lax.axis_size("freq")
    members = lax.axis_size("band")
    rows = pair_density.shape[0]
    freqs, _, vecs, grid_here = trial_vectors.shape
    pair_count = rows * groups * members
    grid_count = grid_here * members
    prefactor = 1.0 / math.sqrt(2.0 * grid_count * pair_count)
    width = freqs * 2 * vecs
    chips = members // 2
    chunks = rows // 8
    piece = rows // chunks
    slot = groups * piece
    dens = jnp.transpose(
        pair_density.reshape(chunks, piece, 2, members, grid_here), (0, 3, 1, 2, 4)
    ).reshape(chunks, members, piece, 2 * grid_here)
    trial = trial_vectors.reshape(width, grid_here)
    dma = pltpu.SemaphoreType.DMA
    vmem = pl.BlockSpec(memory_space=pltpu.VMEM)
    smem = pl.BlockSpec(memory_space=pltpu.SMEM)
    images, sub = pl.pallas_call(
        functools.partial(
            kernel, groups, members, chunks, freqs, vecs, rows, grid_here, prefactor, 1.0 / grid_count
        ),
        out_shape=(
            jax.ShapeDtypeStruct((width, grid_here), F32),
            jax.ShapeDtypeStruct((width, vecs), F32),
        ),
        in_specs=[vmem] * 2 + [smem] * 3 + [vmem],
        out_specs=(vmem, vmem),
        scratch_shapes=[
            pltpu.VMEM((chunks, groups, members, piece, 2 * grid_here), BF16),
            pltpu.VMEM((width, 2 * grid_here), BF16),
            pltpu.VMEM((8, 128), F32),
            pltpu.VMEM((1, width), F32),
            pltpu.VMEM((groups, members, 8, 128), F32),
            pltpu.VMEM((chunks, members * slot, 8), F32),
            pltpu.VMEM((chunks, chips, slot, width), BF16),
            pltpu.VMEM((chunks, chips, slot, width), BF16),
            pltpu.VMEM((2, chips, slot, width), F32),
            pltpu.VMEM((chunks, chips, slot, width), BF16),
            pltpu.VMEM((chunks, chips, slot, width), BF16),
            pltpu.VMEM((chunks, 2, chips, slot, width), BF16),
            pltpu.VMEM((freqs, 2 * vecs, 2 * vecs), F32),
            dma((chunks, members)), dma((chunks, members)),
            dma((chunks, groups, chips)), dma((chunks, groups, chips)),
            dma((members,)), dma((members,)),
            dma((groups,)), dma((groups,)),
            dma((chunks,)), dma((chunks,)),
            dma((chunks, chips)), dma((chunks, chips)),
            dma((chunks, chips)), dma((chunks, chips)),
            dma((chunks,)), dma((chunks,)),
        ],
        compiler_params=pltpu.CompilerParams(
            collective_id=0, has_side_effects=True, vmem_limit_bytes=56 * 1024 * 1024
        ),
    )(dens, trial, frequency, val_energy, cond_energy, pair_index[None, :])
    return (
        images.reshape(freqs, 2, vecs, grid_here),
        sub.reshape(freqs, 2, vecs, vecs),
    )


def solution(mesh):
    return jax.shard_map(
        shards,
        mesh=mesh,
        in_specs=(
            P(("freq", "band"), None, None),
            P("freq", None, None, "band"),
            P("freq"),
            P(),
            P(),
            P(("freq", "band")),
        ),
        out_specs=(P("freq", None, None, "band"), P("freq", None, None, None)),
        check_vma=False,
    )
```

```python
import functools
import math

import jax
import jax.numpy as jnp
from jax import lax
from jax.experimental import pallas as pl
from jax.experimental.pallas import tpu as pltpu
from jax.sharding import PartitionSpec as P

MESH = pl.DeviceIdType.MESH
F32 = jnp.float32
BF16 = jnp.bfloat16


def kernel(
    groups, members, chunks, freqs, vecs, rows, grid_here, prefactor, inv_grid,
    dens, trial, frequency, val_energy, cond_energy, pair_index,
    images, sub,
    held, mix, delta_own, freq_row, deltas, cols, part_out, part_in, own, ring_out, ring_in, scaled, acc,
    sem_as, sem_ar, sem_fs, sem_fr, sem_ds, sem_dr, sem_es, sem_er,
    sem_ps, sem_pr, sem_rs, sem_rr, sem_gs, sem_gr, sem_hs, sem_hr,
):
    f = lax.axis_index("freq")
    b = lax.axis_index("band")
    chips = members // 2
    piece = rows // chunks
    zc = b // 2
    core = b % 2
    width = freqs * 2 * vecs
    chunk_rows = groups * members * piece
    slot = groups * piece
    partner = zc * 2 + (1 - core)

    def remote(src, dst, send, recv, freq_id, band_id):
        return pltpu.make_async_remote_copy(
            src_ref=src, dst_ref=dst, send_sem=send, recv_sem=recv,
            device_id=(freq_id, band_id), device_id_type=MESH,
        )

    barrier = pltpu.get_barrier_semaphore()
    for s in range(1, members):
        pl.semaphore_signal(barrier, inc=1, device_id=(f, (b + s) % members), device_id_type=MESH)
    for s in range(1, groups):
        pl.semaphore_signal(barrier, inc=1, device_id=((f + s) % groups, b), device_id_type=MESH)
    pl.semaphore_wait(barrier, members + groups - 2)

    def waves(c, to):
        return dens.at[c, :, :, pl.ds(pl.multiple_of(to * grid_here, 128), grid_here)]

    sends = []

    def go(copy):
        copy.start()
        sends.append(copy)

    for c in range(chunks):
        pltpu.make_async_copy(waves(c, b), held.at[c, f, b], sem_ar.at[c, b]).start()
        go(remote(waves(c, partner), held.at[c, f, b], sem_as.at[c, 0], sem_ar.at[c, b], f, partner))
    def exchange(c):
        for r in range(1, chips):
            for k in range(2):
                to = (zc + r) % chips * 2 + (core + k) % 2
                go(remote(waves(c, to), held.at[c, f, b], sem_as.at[c, 2 * r + k], sem_ar.at[c, b], f, to))

    cond_count = cond_energy.shape[0]
    val_count = val_energy.shape[0]
    index = pair_index[...]
    rest_index = index
    val_pick = jnp.full(index.shape, val_energy[0], F32)
    for v in range(1, val_count):
        above = index >= v * cond_count
        val_pick = jnp.where(above, val_energy[v], val_pick)
        rest_index = jnp.where(above, index - v * cond_count, rest_index)
    cond_pick = jnp.full(index.shape, cond_energy[0], F32)
    for v in range(1, cond_count):
        cond_pick = jnp.where(rest_index == v, cond_energy[v], cond_pick)
    delta_own[...] = jnp.ones_like(delta_own)
    delta_own[0:1, 0:rows] = cond_pick - val_pick
    for q in range(freqs):
        freq_row[:, q * 2 * vecs : (q + 1) * 2 * vecs] = jnp.full((1, 2 * vecs), frequency[q], F32)
    pltpu.make_async_copy(delta_own, deltas.at[f, b], sem_dr.at[b]).start()
    for s in range(1, members):
        to = (b + s) % members
        go(remote(delta_own, deltas.at[f, b], sem_ds.at[s], sem_dr.at[b], f, to))

    for q in range(freqs):
        lo, hi = q * 2 * vecs, (q * 2 + 1) * vecs
        top = trial[lo : lo + vecs, :]
        low = trial[hi : hi + vecs, :]
        mix[lo : lo + vecs, 0:grid_here] = top
        mix[lo : lo + vecs, grid_here:] = low
        mix[hi : hi + vecs, 0:grid_here] = low
        mix[hi : hi + vecs, grid_here:] = -top

    square_groups = groups == 4
    xx, yy = f % 2, f // 2
    fx, fy = yy * 2 + (1 - xx), (1 - yy) * 2 + xx
    fd = (1 - yy) * 2 + (1 - xx)

    def piece_copy(c, g, z, lane, peer):
        ref = held.at[c, g, pl.ds(2 * z, 2)]
        return remote(ref, ref, sem_fs.at[c, lane, z], sem_fr.at[c, lane, z], peer, b)

    def whole(c, g, lane, peer):
        return remote(held.at[c, g], held.at[c, g], sem_fs.at[c, lane, 0], sem_fr.at[c, lane, 0], peer, b)

    def spread(c, offsets):
        for r in offsets:
            z = (zc + r) % chips
            for k in range(2):
                j = z * 2 + k
                pltpu.make_async_copy(waves(c, 0), held.at[c, f, j], sem_ar.at[c, j]).wait()
            if square_groups:
                go(piece_copy(c, f, z, 0, fx))
                go(piece_copy(c, f, z, 1, fy))
        if not square_groups and offsets[-1] == chips - 1:
            for s in range(1, groups):
                go(whole(c, f, s, (f + s) % groups))

    def relay(c):
        if square_groups:
            for r in range(chips):
                z = (zc + r) % chips
                if r % 2 == 0:
                    piece_copy(c, fx, z, 0, fx).wait_recv()
                    go(piece_copy(c, fx, z, 2, fy))
                else:
                    piece_copy(c, fy, z, 1, fy).wait_recv()
                    go(piece_copy(c, fy, z, 3, fx))

    def arrive(c):
        if square_groups:
            for r in range(chips):
                z = (zc + r) % chips
                if r % 2 == 0:
                    piece_copy(c, fy, z, 1, fy).wait_recv()
                    piece_copy(c, fd, z, 2, fy).wait_recv()
                else:
                    piece_copy(c, fx, z, 0, fx).wait_recv()
                    piece_copy(c, fd, z, 3, fx).wait_recv()
        else:
            for s in range(1, groups):
                src = (f + groups - s) % groups
                whole(c, src, s, src).wait_recv()

    def pass_deltas():
        for j in range(members):
            pltpu.make_async_copy(delta_own, deltas.at[f, j], sem_dr.at[j]).wait()
        for s in range(1, groups):
            go(remote(deltas.at[f], deltas.at[f], sem_es.at[s], sem_er.at[s], (f + s) % groups, b))

    def columns():
        for s in range(1, groups):
            src = (f + groups - s) % groups
            remote(deltas.at[src], deltas.at[src], sem_es.at[s], sem_er.at[s], src, b).wait_recv()
        for g in range(groups):
            for j in range(members):
                turned = jnp.transpose(deltas[g, j])
                at = (g * members + j) * piece
                for c in range(chunks):
                    cols[c, at : at + piece, :] = turned[c * piece : (c + 1) * piece, :]

    def weights(column):
        ratio = column / (column * column + freq_row[...] * freq_row[...])
        return (-4.0 * prefactor * ratio).astype(BF16).astype(F32)

    def cross(j):
        arrive(j)
        over_grid = (((1,), (1,)), ((), ()))
        real = held[j, :, :, 0].reshape(chunk_rows, grid_here)
        imag = held[j, :, :, 1].reshape(chunk_rows, grid_here)
        own[...] = (
            lax.dot_general(real, mix[:, 0:grid_here], over_grid, preferred_element_type=F32)
            + lax.dot_general(imag, mix[:, grid_here:], over_grid, preferred_element_type=F32)
        ).reshape(2, chips, chunk_rows // members, width)
        part_out[j] = own[1 - core].astype(BF16)
        go(remote(part_out.at[j], part_in.at[j], sem_ps.at[j], sem_pr.at[j], f, partner))
        remote(part_out.at[j], part_in.at[j], sem_ps.at[j], sem_pr.at[j], f, partner).wait_recv()
        total = own[core] + part_in[j].astype(F32)
        ring_out[j] = total.astype(BF16)
        for s in range(1, chips):
            to = (zc + s) % chips
            go(remote(ring_out.at[j, to], ring_in.at[j, s], sem_rs.at[j, s], sem_rr.at[j, s], f, to * 2 + core))

    def scale(j):
        total = ring_out[j, zc].astype(F32)
        for s in range(1, chips):
            src = (zc + chips - s) % chips
            remote(ring_out.at[j, zc], ring_in.at[j, s], sem_rs.at[j, s], sem_rr.at[j, s], f, src * 2 + core).wait_recv()
            total = total + ring_in[j, s].astype(F32)
        q = core * chips + zc
        column = cols[j, pl.ds(pl.multiple_of(q * slot, 8), slot), 0:1]
        scaled[j, core, zc] = (weights(column) * total).astype(BF16)
        for s in range(1, chips):
            to = (zc + s) % chips
            go(remote(scaled.at[j, core, zc], scaled.at[j, core, zc], sem_gs.at[j, s], sem_gr.at[j, s], f, to * 2 + core))

    def share(j):
        for s in range(1, chips):
            src = (zc + chips - s) % chips
            remote(scaled.at[j, core, src], scaled.at[j, core, src], sem_gs.at[j, s], sem_gr.at[j, s], f, src * 2 + core).wait_recv()
        go(remote(scaled.at[j, core], scaled.at[j, core], sem_hs.at[j], sem_hr.at[j], f, partner))

    def image(j):
        remote(scaled.at[j, 1 - core], scaled.at[j, 1 - core], sem_hs.at[j], sem_hr.at[j], f, partner).wait_recv()
        flat = scaled[j].reshape(chunk_rows, width)
        flat32 = flat.astype(F32)
        lane = lax.broadcasted_iota(jnp.int32, (1, 2 * vecs), 1)
        sign = jnp.where(lane < vecs, -1.0, 1.0)
        turned = jnp.concatenate(
            [
                pltpu.roll(flat32[:, q * 2 * vecs : (q + 1) * 2 * vecs], vecs, 1) * sign
                for q in range(freqs)
            ],
            axis=1,
        ).astype(BF16)
        over_rows = (((0,), (0,)), ((), ()))
        real = held[j, :, :, 0].reshape(chunk_rows, grid_here)
        imag = held[j, :, :, 1].reshape(chunk_rows, grid_here)
        term = lax.dot_general(flat, real, over_rows, preferred_element_type=F32) + lax.dot_general(
            turned, imag, over_rows, preferred_element_type=F32
        )
        column = cols[j, :, 0:1]
        crossing = (flat32 / weights(column)).astype(BF16)
        for q in range(freqs):
            lo, hi = q * 2 * vecs, (q + 1) * 2 * vecs
            square = lax.dot_general(
                crossing[:, lo:hi], flat[:, lo:hi], over_rows, preferred_element_type=F32
            )
            if j == 0:
                acc[q] = square
            else:
                acc[q] = acc[q] + square
        if j == 0:
            images[...] = term
        else:
            images[...] = images[...] + term

    exchange(0)
    for c in range(chunks):
        spread(c, (0,))
    pass_deltas()
    for t in range(chunks + 4):
        if t + 1 < chunks:
            exchange(t + 1)
        if t < chunks:
            spread(t, range(1, chips))
        if t == 0:
            columns()
        if 0 <= t - 1 < chunks:
            relay(t - 1)
        if 0 <= t - 3 < chunks:
            scale(t - 3)
        if 0 <= t - 2 < chunks:
            cross(t - 2)
        if 0 <= t - 4 < chunks:
            share(t - 4)
            image(t - 4)

    for q in range(freqs):
        square = acc[q]
        lo, hi = q * 2 * vecs, (q * 2 + 1) * vecs
        sub[lo : lo + vecs, :] = (square[0:vecs, 0:vecs] + square[vecs:, vecs:]) * inv_grid
        sub[hi : hi + vecs, :] = (square[0:vecs, vecs:] - square[vecs:, 0:vecs]) * inv_grid

    for copy in sends:
        copy.wait_send()


def shards(pair_density, trial_vectors, frequency, val_energy, cond_energy, pair_index):
    groups = lax.axis_size("freq")
    members = lax.axis_size("band")
    rows = pair_density.shape[0]
    freqs, _, vecs, grid_here = trial_vectors.shape
    pair_count = rows * groups * members
    grid_count = grid_here * members
    prefactor = 1.0 / math.sqrt(2.0 * grid_count * pair_count)
    width = freqs * 2 * vecs
    chips = members // 2
    chunks = rows // 8
    piece = rows // chunks
    slot = groups * piece
    dens = jnp.transpose(
        pair_density.reshape(chunks, piece, 2, grid_count), (0, 2, 1, 3)
    )
    trial = trial_vectors.reshape(width, grid_here)
    dma = pltpu.SemaphoreType.DMA
    vmem = pl.BlockSpec(memory_space=pltpu.VMEM)
    smem = pl.BlockSpec(memory_space=pltpu.SMEM)
    images, sub = pl.pallas_call(
        functools.partial(
            kernel, groups, members, chunks, freqs, vecs, rows, grid_here, prefactor, 1.0 / grid_count
        ),
        out_shape=(
            jax.ShapeDtypeStruct((width, grid_here), F32),
            jax.ShapeDtypeStruct((width, vecs), F32),
        ),
        in_specs=[vmem] * 2 + [smem] * 3 + [vmem],
        out_specs=(vmem, vmem),
        scratch_shapes=[
            pltpu.VMEM((chunks, groups, members, 2, piece, grid_here), BF16),
            pltpu.VMEM((width, 2 * grid_here), BF16),
            pltpu.VMEM((8, 128), F32),
            pltpu.VMEM((1, width), F32),
            pltpu.VMEM((groups, members, 8, 128), F32),
            pltpu.VMEM((chunks, members * slot, 8), F32),
            pltpu.VMEM((chunks, chips, slot, width), BF16),
            pltpu.VMEM((chunks, chips, slot, width), BF16),
            pltpu.VMEM((2, chips, slot, width), F32),
            pltpu.VMEM((chunks, chips, slot, width), BF16),
            pltpu.VMEM((chunks, chips, slot, width), BF16),
            pltpu.VMEM((chunks, 2, chips, slot, width), BF16),
            pltpu.VMEM((freqs, 2 * vecs, 2 * vecs), F32),
            dma((chunks, members)), dma((chunks, members)),
            dma((chunks, groups, chips)), dma((chunks, groups, chips)),
            dma((members,)), dma((members,)),
            dma((groups,)), dma((groups,)),
            dma((chunks,)), dma((chunks,)),
            dma((chunks, chips)), dma((chunks, chips)),
            dma((chunks, chips)), dma((chunks, chips)),
            dma((chunks,)), dma((chunks,)),
        ],
        compiler_params=pltpu.CompilerParams(
            collective_id=0, has_side_effects=True, vmem_limit_bytes=56 * 1024 * 1024
        ),
    )(dens, trial, frequency, val_energy, cond_energy, pair_index[None, :])
    return (
        images.reshape(freqs, 2, vecs, grid_here),
        sub.reshape(freqs, 2, vecs, vecs),
    )


def solution(mesh):
    return jax.shard_map(
        shards,
        mesh=mesh,
        in_specs=(
            P(("freq", "band"), None, None),
            P("freq", None, None, "band"),
            P("freq"),
            P(),
            P(),
            P(("freq", "band")),
        ),
        out_specs=(P("freq", None, None, "band"), P("freq", None, None, None)),
        check_vma=False,
    )
```
